128 devices in a mesh: dp: 16 (over x, y), mp: 8 (over z, core).
Axes of the slice: x: 4, y: 4, z: 4, core: 2. Of those that a mesh axis runs over, the one named last changes fastest.
Arguments:
- patches: bfloat16 [768, 64, 1024], P(('dp', 'mp')), may hold values from -6 to 6
- gain_first: float32 [1024], replicated, may hold values from 0.1 to 1.9
- joint_weight: bfloat16 [1024, 3, 1024], P('dp', None, 'mp'), may hold values from -0.1875 to 0.1875
- head_scale: float32 [16], P('mp'), may hold values from 2 to 32
- output_weight: bfloat16 [1024, 1024], P('mp', 'dp'), may hold values from -0.1875 to 0.1875
- gain_second: float32 [1024], replicated, may hold values from 0.3 to 3
- up_weight: bfloat16 [1024, 4096], P('dp', 'mp'), may hold values from -0.1875 to 0.1875
- down_weight: bfloat16 [4096, 1024], P('mp', 'dp'), may hold values from -0.09375 to 0.09375
- gain_final: float32 [1024], replicated, may hold values from 0.1 to 1.9
- project_weight: bfloat16 [1024, 768], replicated, may hold values from -0.1875 to 0.1875
- text_bank: bfloat16 [12288, 768], P(('dp', 'mp')), may hold values from -20000 to 20000
- captions: int32 [768], replicated, may hold values from 0 to 12287
- reference_loss: float32 [768], P(('dp', 'mp')), may hold values from 2 to 20
Outputs:
- learnability: float32 [768], P(('dp', 'mp'))
The draws below stay inside these ranges and needn't reach their ends.
All inputs are finite; a program needn't handle non-finite values.
Results may differ from the reference program's by a relative error of at most 0.018.
Values may be sent and summed in bfloat16 or wider, within the bound.
No kernel may reach another device: no remote copies, remote signals or barrier semaphores. Data moves between devices by JAX's collectives and lax.ppermute only.
A program may use at most 128 MiB of HBM per device.

```python
import math
import jax
import jax.numpy as jnp
from jax import lax

D = 1024
H = 16
HD = 64
FF = 4096
P_SIZE = 64
E = 768
IMG_DEV = 48
IMAGES = 768
TEXTS = 12288
N_MP = 8


def draw_text_bank(key, part):
    key_dir = jax.random.fold_in(key, 11)
    key_len = jax.random.fold_in(key, 12)
    direction = jax.random.truncated_normal(key_dir, -4.0, 4.0, (TEXTS, E), jnp.float32)
    growth = jnp.exp(math.log(3.0) * jnp.arange(TEXTS, dtype=jnp.float32)[:, None] / max(TEXTS - 1, 1))
    lengths = jnp.exp(jax.random.uniform(key_len, (TEXTS, 1), jnp.float32, math.log(12.0), math.log(120.0))) * growth
    return (direction * lengths / math.sqrt(E)).astype(jnp.bfloat16)


def place_ends(array, rng, least, largest):
    spot = [jax.random.randint(jax.random.fold_in(rng, axis), (), 0, length) for axis, length in enumerate(array.shape)]
    widest = array.shape.index(max(array.shape))
    neighbour = spot[:widest] + [(spot[widest] + 1) % array.shape[widest]] + spot[widest + 1:]
    return array.at[tuple(spot)].set(least).at[tuple(neighbour)].set(largest)


def level_of(key, extent, cuts, least, largest):
    loudness, own = 1.0, jax.random.fold_in(key, 6)
    for axis_at, shards_of in cuts:
        draws = jnp.exp(jax.random.uniform(jax.random.fold_in(own, axis_at), (shards_of,), jnp.float32, least / len(cuts), largest / len(cuts)))
        loudness = loudness * jnp.repeat(draws, extent[axis_at] // shards_of).reshape([-1 if axis == axis_at else 1 for axis in range(len(extent))])
    return loudness


def centred(stream_key, dims, width, limit, pieces=(), kind=jnp.bfloat16):
    array = jax.random.normal(stream_key, dims, jnp.float32) * width
    if len(pieces) > 0:
        array = level_of(stream_key, dims, pieces, -0.22, 0.18) * array
    return jnp.clip(array, min=-limit, max=limit).astype(kind)


def setup_inputs(seed: int = 0) -> dict:
    key_of = jax.random.split(jax.random.key(seed), 14)
    patches = centred(key_of[0], (IMAGES, P_SIZE, D), 1.0, 6.0, ((0, 128),))
    gain_first = jnp.clip(1.0 + 0.18 * jax.random.normal(key_of[1], (D,), jnp.float32), 0.1, 1.9)
    joint_weight = centred(key_of[2], (D, 3, D), D ** -0.5, 0.1875, ((0, 16), (2, 8)))
    head_scale = jnp.clip(jnp.exp(math.log(32.0) - 2.7725887 * jax.random.uniform(key_of[3], (H,), jnp.float32) ** level_of(key_of[3], (H,), ((0, 8),), -0.2, 0.2)), 2.0, 32.0)
    output_weight = centred(key_of[4], (D, D), D ** -0.5, 0.1875, ((0, 8), (1, 16)))
    gain_second = jnp.clip(jnp.exp(jax.random.uniform(key_of[5], (D,), jnp.float32, math.log(0.3), math.log(3.0))), 0.3, 3.0)
    up_weight = centred(key_of[6], (D, FF), D ** -0.5, 0.1875, ((0, 16), (1, 8)))
    down_weight = centred(key_of[7], (FF, D), FF ** -0.5, 0.09375, ((0, 8), (1, 16)))
    gain_final = jnp.clip(1.0 + 0.18 * jax.random.normal(key_of[8], (D,), jnp.float32), 0.1, 1.9)
    project_weight = centred(key_of[9], (D, E), D ** -0.5, 0.1875)
    text_bank = draw_text_bank(jax.random.fold_in(key_of[13], 71), 0)
    captions = place_ends(jax.random.randint(key_of[11], (IMAGES,), 0, TEXTS), jax.random.fold_in(key_of[11], 1), 0, TEXTS - 1).astype(jnp.int32)
    reference_loss = jnp.clip(2.0 + 18.0 * jax.random.uniform(key_of[12], (IMAGES,), jnp.float32) ** level_of(key_of[12], (IMAGES,), ((0, 128),), -0.2, 0.2), 2.0, 20.0)
    return dict(patches=patches, gain_first=gain_first, joint_weight=joint_weight, head_scale=head_scale, output_weight=output_weight, gain_second=gain_second, up_weight=up_weight, down_weight=down_weight, gain_final=gain_final, project_weight=project_weight, text_bank=text_bank, captions=captions, reference_loss=reference_loss)


def layer_norm(values, gain):
    centre = values - lax.optimization_barrier(jnp.mean(values, axis=-1, keepdims=True))
    spread = lax.optimization_barrier(jnp.mean(centre * centre, axis=-1, keepdims=True))
    return centre * lax.rsqrt(spread + 1e-06) * gain

def unit_rows(values):
    return values * lax.rsqrt(lax.optimization_barrier(jnp.sum(values * values, axis=-1, keepdims=True)) + 1e-06)

def grouped_product(left_rows, right_cols, groups):
    group_width = left_rows.shape[1] // groups
    totals = jnp.zeros((left_rows.shape[0], right_cols.shape[1]), jnp.float32)
    for index_group in range(groups):
        lower = index_group * group_width
        partial_value = jnp.dot(left_rows[:, lower:lower + group_width], right_cols[lower:lower + group_width], preferred_element_type=jnp.float32)
        rounded = lax.optimization_barrier(partial_value.astype(jnp.bfloat16))
        totals = totals + rounded.astype(jnp.float32)
    return totals

def reference(patches, gain_first, joint_weight, head_scale, output_weight, gain_second, up_weight, down_weight, gain_final, project_weight, text_bank, captions, reference_loss):

    def encode(image_block):
        amount = image_block.shape[0]
        residual = image_block.astype(jnp.float32).reshape(amount * P_SIZE, D)
        normed_first = layer_norm(residual, gain_first).astype(jnp.bfloat16)
        joint = jnp.dot(normed_first, joint_weight.reshape(D, 3 * D), preferred_element_type=jnp.float32)
        joint = joint.reshape(amount, P_SIZE, 3, H, HD)
        queries = unit_rows(joint[:, :, 0]).astype(jnp.bfloat16)
        key_rows = unit_rows(joint[:, :, 1]).astype(jnp.bfloat16)
        value_rows = joint[:, :, 2].astype(jnp.bfloat16)
        scores = jnp.einsum('bqhd,bkhd->bhqk', queries.astype(jnp.float32), key_rows.astype(jnp.float32))
        exponent = jnp.exp(scores * head_scale[None, :, None, None])
        attention = (exponent / lax.optimization_barrier(jnp.sum(exponent, axis=-1, keepdims=True))).astype(jnp.bfloat16)
        head_out = jnp.einsum('bhqk,bkhd->bqhd', attention.astype(jnp.float32), value_rows.astype(jnp.float32))
        head_out = head_out.astype(jnp.bfloat16).reshape(amount * P_SIZE, D)
        residual_two = residual + grouped_product(head_out, output_weight, N_MP)
        normed_second = layer_norm(residual_two, gain_second).astype(jnp.bfloat16)
        upper = jnp.dot(normed_second, up_weight, preferred_element_type=jnp.float32)
        hidden = jax.nn.gelu(upper, approximate=False).astype(jnp.bfloat16)
        feed = grouped_product(hidden, down_weight, N_MP)
        pooled = lax.optimization_barrier(jnp.mean((residual_two + feed).reshape(amount, P_SIZE, D), axis=1))
        pooled_norm = layer_norm(pooled, gain_final).astype(jnp.bfloat16)
        embedded = jnp.dot(pooled_norm, project_weight, preferred_element_type=jnp.float32)
        return unit_rows(embedded).astype(jnp.bfloat16)
    image_blocks = patches.reshape(IMAGES // IMG_DEV, IMG_DEV, P_SIZE, D)
    image_units = lax.map(encode, image_blocks).reshape(IMAGES, E)
    logits = jnp.dot(image_units, text_bank.T, preferred_element_type=jnp.float32)
    highest = lax.optimization_barrier(jnp.max(logits, axis=1))
    totals = lax.optimization_barrier(jnp.sum(jnp.exp(logits - highest[:, None]), axis=1))
    matched = jnp.take_along_axis(logits, captions.astype(jnp.int32)[:, None], axis=1)[:, 0]
    loss = highest + jnp.log(totals) - matched
    return loss - reference_loss
```

```python
import jax
import jax.numpy as jnp
from jax import lax
from jax.experimental import pallas as pl
from jax.experimental.pallas import tpu as pltpu
from jax.sharding import PartitionSpec as P


AXES = ("dp", "mp")
DEVICES = [(x, y, z, c) for x in range(4) for y in range(4) for z in range(4) for c in range(2)]
F32 = jnp.float32
BF16 = jnp.bfloat16
NT = (((1,), (1,)), ((), ()))


def device_id(x, y, z, c):
    return x * 32 + y * 8 + z * 2 + c


def shift_pairs(axis, step):
    pairs = []
    for place in DEVICES:
        goal = list(place)
        goal[axis] = (goal[axis] + (step if place[3] == 0 else -step)) % 4
        pairs.append((device_id(*place), device_id(*goal)))
    return pairs


SWAP = [(i, i ^ 1) for i in range(128)]


def swapped(array):
    return lax.ppermute(array, AXES, SWAP)


def ring(array, axis):
    ahead = lax.ppermute(array, AXES, shift_pairs(axis, 1))
    behind = lax.ppermute(array, AXES, shift_pairs(axis, -1))
    far = lax.ppermute(ahead, AXES, shift_pairs(axis, 1))
    return [array, ahead, behind, far]


def call(body, outs, args, grid=(1,), ins=None, out_specs=None, scratch=(), prefetch=0, limit=32, name=None):
    whole = lambda s: pl.BlockSpec(s, lambda *_: (0,) * len(s))
    ins = ins or [None] * (len(args) - prefetch)
    ins = [b or whole(a.shape) for b, a in zip(ins, args[prefetch:])]
    out_specs = out_specs or [whole(o.shape) for o in outs]
    return pl.pallas_call(
        body,
        out_shape=outs,
        grid_spec=pltpu.PrefetchScalarGridSpec(
            num_scalar_prefetch=prefetch, grid=grid, in_specs=ins, out_specs=out_specs, scratch_shapes=list(scratch)
        ),
        compiler_params=pltpu.CompilerParams(vmem_limit_bytes=limit << 20),
        name=name,
    )(*args)


def norm_rows(values, gain):
    centre = values - jnp.mean(values, axis=-1, keepdims=True)
    spread = jnp.mean(centre * centre, axis=-1, keepdims=True)
    return centre * lax.rsqrt(spread + 1e-06) * gain


def split(values):
    high = values.astype(BF16)
    return high, (values - high.astype(F32)).astype(BF16)


def block_ones(size, block):
    row = lax.broadcasted_iota(jnp.int32, (size, size), 0) // block
    col = lax.broadcasted_iota(jnp.int32, (size, size), 1) // block
    return (row == col).astype(F32).astype(BF16)


def norm_kernel(own, other, gain, own_out, other_out):
    own_out[...] = norm_rows(own[...].astype(F32), gain[...]).astype(BF16)
    other_out[...] = norm_rows(other[...].astype(F32), gain[...]).astype(BF16)


def attend_kernel(place, own, other, piece, out, weight):
    for j in range(16):
        at = pl.multiple_of(place[j] * 64, 64)
        weight[pl.ds(at, 64), :] = piece[j * 64 : (j + 1) * 64, 0:384]
    scale = jnp.sum(piece[1024:1040, 0:128].astype(F32), axis=0, keepdims=True)
    ones = block_ones(256, 64)
    lane = lax.broadcasted_iota(jnp.int32, (64, 128), 1)
    first = lane < 64
    nil = jnp.zeros((64, 128), F32)
    for side, rows in enumerate((own, other)):
        joint = jnp.dot(rows[...], weight[...], preferred_element_type=F32)
        pair = joint[:, 0:256]
        high, low = split(pair * pair)
        squares = jnp.dot(high, ones, preferred_element_type=F32) + jnp.dot(low, ones, preferred_element_type=F32)
        unit = pair * lax.rsqrt(squares + 1e-06)
        for i in range(6):
            at = slice(i * 64, (i + 1) * 64)
            query = unit[at, 0:128].astype(BF16)
            key = unit[at, 128:256]
            value = joint[at, 256:384]
            keys = jnp.concatenate([jnp.where(first, key, nil), jnp.where(first, nil, key)], axis=0).astype(BF16)
            values = jnp.concatenate([jnp.where(first, value, nil), jnp.where(first, nil, value)], axis=0).astype(BF16)
            scores = lax.dot_general(query, keys, NT, preferred_element_type=F32)
            weights = jnp.exp(scores * scale).astype(BF16)
            mixed = jnp.dot(weights, values, preferred_element_type=F32)
            total = jnp.dot(weights, ones[0:128, 0:128], preferred_element_type=F32)
            out[side * 384 + i * 64 : side * 384 + (i + 1) * 64, :] = (mixed / total).astype(BF16)


def output_kernel(place, h0, h1, h2, h3, p0, p1, p2, p3, own, other, weight):
    for r, piece in enumerate((p0, p1, p2, p3)):
        for j in range(16):
            at = pl.multiple_of(place[j] * 64, 64)
            weight[pl.ds(at, 64), r * 128 : (r + 1) * 128] = piece[j * 64 : (j + 1) * 64, :]
    heads = jnp.concatenate([h0[...], h1[...], h2[...], h3[...]], axis=1)
    own[...] = lax.dot_general(heads[0:384], weight[...], NT, preferred_element_type=F32)
    other[...] = lax.dot_general(heads[384:768], weight[...], NT, preferred_element_type=F32).astype(BF16)


def residual_kernel(patches, own, other, gain, normed, pooled):
    residual = patches[...].astype(F32) + own[...] + other[...].astype(F32)
    normed[...] = norm_rows(residual, gain[...]).astype(BF16)
    pooled[0:6] = jnp.sum(residual.reshape(6, 64, 1024), axis=1) * (1.0 / 64)
    pooled[6:8] = jnp.zeros((2, 1024), F32)


def up_kernel(place, own, other, p0, p1, p2, p3, mean, weight):
    for r, piece in enumerate((p0, p1, p2, p3)):
        for j in range(4):
            at = pl.multiple_of(place[r * 4 + j] * 64, 64)
            weight[pl.ds(at, 64), :] = piece[j * 64 : (j + 1) * 64, :]
    for side, rows in enumerate((own, other)):
        upper = jnp.dot(rows[...], weight[...], preferred_element_type=F32)
        hidden = (0.5 * upper * (1.0 + lax.erf(upper * 0.7071067811865476))).astype(BF16).astype(F32)
        mean[side * 8 : side * 8 + 6, :] = jnp.sum(hidden.reshape(6, 64, 512), axis=1) * (1.0 / 64)
        mean[side * 8 + 6 : side * 8 + 8, :] = jnp.zeros((2, 512), F32)


def down_kernel(place, mean, p0, p1, p2, p3, own, other, weight):
    for r, piece in enumerate((p0, p1, p2, p3)):
        for j in range(4):
            at = pl.multiple_of(place[r * 4 + j] * 64, 64)
            for k in range(4):
                weight[pl.ds(at, 64), k * 512 : (k + 1) * 512] = piece[(j * 4 + k) * 64 : (j * 4 + k + 1) * 64, :]
    high, low = split(mean[...])
    both = jnp.concatenate([high, low], axis=0)
    product = lax.dot_general(both, weight[...], NT, preferred_element_type=F32)
    product = product[0:16] + product[16:32]
    own[...] = product[0:8]
    other[...] = product[8:16]


def final_kernel(pooled, own, other, gain, project, units):
    total = pooled[...] + own[...] + other[...]
    normed = norm_rows(total, gain[...]).astype(BF16)
    embedded = jnp.dot(normed, project[...], preferred_element_type=F32)
    units[...] = (
        embedded * lax.rsqrt(jnp.sum(embedded * embedded, axis=-1, keepdims=True) + 1e-06)
    ).astype(BF16)


def logits_kernel(units, texts, wanted, ids, out):
    logits = lax.dot_general(units[...], texts[...], NT, preferred_element_type=F32)
    highest = jnp.max(logits, axis=1, keepdims=True)
    total = jnp.sum(jnp.exp(logits - highest), axis=1, keepdims=True)
    matched = jnp.sum(jnp.where(wanted[...] == ids[...], logits, 0.0), axis=1, keepdims=True)
    lane = lax.broadcasted_iota(jnp.int32, (128, 128), 1)
    out[...] = jnp.where(lane == 0, highest, jnp.where(lane == 1, total, matched))


def loss_kernel(parts, loss):
    highest = parts[0]
    for i in range(1, 16):
        highest = jnp.maximum(highest, parts[i])
    highest = highest[:, 0:1]
    total = jnp.zeros((8, 1), F32)
    matched = jnp.zeros((8, 1), F32)
    for i in range(16):
        part = parts[i]
        total = total + part[:, 1:2] * jnp.exp(part[:, 0:1] - highest)
        matched = matched + part[:, 2:3]
    loss[...] = jnp.broadcast_to(highest + jnp.log(total) - matched, (8, 128))


def shards(
    patches,
    gain_first,
    joint_weight,
    head_scale,
    output_weight,
    gain_second,
    up_weight,
    down_weight,
    gain_final,
    project_weight,
    text_bank,
    captions,
    reference_loss,
):
    dp, mp = lax.axis_index("dp"), lax.axis_index("mp")
    ix, iy, iz, core = dp // 4, dp % 4, mp // 2, mp % 2
    sign = 1 - 2 * core
    offsets = jnp.stack([0 * sign, -sign, sign, 0 * sign + 2])
    rx, ry, rz = (ix + offsets + 4) % 4, (iy + offsets + 4) % 4, (iz + offsets + 4) % 4
    by_y_x = (rx[None, :] * 4 + ry[:, None]).reshape(16).astype(jnp.int32)
    by_x_y = (rx[:, None] * 4 + ry[None, :]).reshape(16).astype(jnp.int32)

    rows = patches.reshape(384, 1024)
    rows_other = swapped(rows)

    shard_a = jnp.concatenate([joint_weight.reshape(64, 384), output_weight.T], axis=1)
    shard_b = up_weight
    shard_c = down_weight.T

    def joined(blocks):
        return jnp.concatenate(blocks, axis=0)

    first_a = joined(ring(shard_a, 0))
    first_b = joined(ring(shard_b, 1))
    first_c = joined(ring(shard_c, 2))
    second_a = joined(ring(first_a, 1))
    second_b = joined(ring(first_b, 2))
    second_c = joined(ring(first_c, 0))
    lanes = jnp.repeat(head_scale, 64)
    high = lax.reduce_precision(lanes, 8, 7)
    middle = lax.reduce_precision(lanes - high, 8, 7)
    low = lanes - high - middle
    scale_rows = jnp.pad(jnp.stack([high, middle, low]), ((0, 13), (0, 384))).astype(BF16)
    pieces_a = ring(jnp.concatenate([second_a, scale_rows], axis=0), 2)
    pieces_b = ring(second_b, 0)
    pieces_c = ring(second_c, 1)

    sds = jax.ShapeDtypeStruct
    gain_row = gain_first.reshape(1, 1024)
    normed_own, normed_other = call(
        norm_kernel, [sds((384, 1024), BF16)] * 2, [rows, rows_other, gain_row], name="norm_first"
    )
    heads = [
        call(
            attend_kernel,
            [sds((768, 128), BF16)],
            [by_y_x, normed_own, normed_other, piece],
            scratch=[pltpu.VMEM((1024, 384), BF16)],
            prefetch=1,
            name="attend",
        )[0]
        for piece in pieces_a
    ]
    last = pl.BlockSpec((1040, 128), lambda *_: (0, 3))
    part_own, part_other = call(
        output_kernel,
        [sds((384, 1024), F32), sds((384, 1024), BF16)],
        [by_y_x, *heads, *pieces_a],
        ins=[None] * 4 + [last] * 4,
        scratch=[pltpu.VMEM((1024, 512), BF16)],
        prefetch=1,
        name="output",
    )
    normed_two, pooled = call(
        residual_kernel,
        [sds((384, 1024), BF16), sds((8, 1024), F32)],
        [rows, part_own, swapped(part_other), gain_second.reshape(1, 1024)],
        name="residual",
    )
    quarter = pl.BlockSpec((256, 512), lambda i, *_: (i, 0))
    mean = call(
        up_kernel,
        [sds((16, 2048), F32)],
        [by_x_y, normed_two, swapped(normed_two), *pieces_b],
        grid=(4,),
        ins=[None] * 2 + [quarter] * 4,
        out_specs=[pl.BlockSpec((16, 512), lambda i, *_: (0, i))],
        scratch=[pltpu.VMEM((1024, 512), BF16)],
        prefetch=1,
        name="up",
    )[0]
    feed_own, feed_other = call(
        down_kernel,
        [sds((8, 1024), F32)] * 2,
        [by_y_x, mean, *pieces_c],
        scratch=[pltpu.VMEM((1024, 2048), BF16)],
        prefetch=1,
        name="down",
    )
    units = call(
        final_kernel,
        [sds((8, 768), BF16)],
        [pooled, feed_own, swapped(feed_other), gain_final.reshape(1, 1024), project_weight],
        name="final",
    )[0]

    texts_own = joined(ring(text_bank, 2))
    texts = jnp.concatenate([texts_own, swapped(texts_own)], axis=0)
    rz_other = (iz - offsets + 4) % 4
    holders = jnp.concatenate([rz * 2 + core, rz_other * 2 + (1 - core)])
    ids = ((dp * 8 + holders)[:, None] * 96 + jnp.arange(96)[None, :]).reshape(1, 768).astype(jnp.int32)
    wanted = lax.dynamic_slice_in_dim(captions.reshape(16, 8, 6), mp, 1, axis=1)[:, 0]
    wanted = jnp.pad(wanted, ((0, 0), (0, 2)), constant_values=-1).reshape(128, 1)

    everyone = lax.all_to_all(jnp.broadcast_to(units[None], (16, 8, 768)), "dp", 0, 0, tiled=True)
    parts = call(
        logits_kernel,
        [sds((128, 128), F32)],
        [everyone.reshape(128, 768), texts, wanted, ids],
        name="logits",
    )[0]
    parts = lax.all_to_all(parts.reshape(16, 8, 128), "dp", 0, 0, tiled=True)
    loss = call(loss_kernel, [sds((8, 128), F32)], [parts], name="loss")[0]
    return loss[0:6, 0] - reference_loss


def solution(mesh):
    placed = (
        P(("dp", "mp"), None, None),
        P(),
        P("dp", None, "mp"),
        P("mp"),
        P("mp", "dp"),
        P(),
        P("dp", "mp"),
        P("mp", "dp"),
        P(),
        P(),
        P(("dp", "mp"), None),
        P(),
        P(("dp", "mp")),
    )
    return jax.shard_map(shards, mesh=mesh, in_specs=placed, out_specs=P(("dp", "mp")), check_vma=False)
```

```python
import jax
import jax.numpy as jnp
from jax import lax
from jax.experimental import pallas as pl
from jax.experimental.pallas import tpu as pltpu
from jax.sharding import PartitionSpec as P


AXES = ("dp", "mp")
DEVICES = [(x, y, z, c) for x in range(4) for y in range(4) for z in range(4) for c in range(2)]
F32 = jnp.float32
BF16 = jnp.bfloat16
NT = (((1,), (1,)), ((), ()))


def device_id(x, y, z, c):
    return x * 32 + y * 8 + z * 2 + c


def shift_pairs(axis, step):
    pairs = []
    for place in DEVICES:
        goal = list(place)
        goal[axis] = (goal[axis] + (step if place[3] == 0 else -step)) % 4
        pairs.append((device_id(*place), device_id(*goal)))
    return pairs


SWAP = [(i, i ^ 1) for i in range(128)]


def swapped(array):
    return lax.ppermute(array, AXES, SWAP)


def ring(array, axis):
    ahead = lax.ppermute(array, AXES, shift_pairs(axis, 1))
    behind = lax.ppermute(array, AXES, shift_pairs(axis, -1))
    far = lax.ppermute(ahead, AXES, shift_pairs(axis, 1))
    return [array, ahead, behind, far]


def call(body, outs, args, grid=(1,), ins=None, out_specs=None, scratch=(), prefetch=0, limit=16):
    whole = lambda s: pl.BlockSpec(s, lambda *_: (0,) * len(s))
    ins = ins or [None] * (len(args) - prefetch)
    ins = [b or whole(a.shape) for b, a in zip(ins, args[prefetch:])]
    out_specs = out_specs or [whole(o.shape) for o in outs]
    return pl.pallas_call(
        body,
        out_shape=outs,
        grid_spec=pltpu.PrefetchScalarGridSpec(
            num_scalar_prefetch=prefetch, grid=grid, in_specs=ins, out_specs=out_specs, scratch_shapes=list(scratch)
        ),
        compiler_params=pltpu.CompilerParams(vmem_limit_bytes=limit << 20),
    )(*args)


def norm_rows(values, gain):
    centre = values - jnp.mean(values, axis=-1, keepdims=True)
    spread = jnp.mean(centre * centre, axis=-1, keepdims=True)
    return centre * lax.rsqrt(spread + 1e-06) * gain


def split(values):
    high = values.astype(BF16)
    return high, (values - high.astype(F32)).astype(BF16)


def block_ones(size, block):
    row = lax.broadcasted_iota(jnp.int32, (size, size), 0) // block
    col = lax.broadcasted_iota(jnp.int32, (size, size), 1) // block
    return (row == col).astype(F32).astype(BF16)


def norm_kernel(own, other, gain, own_out, other_out):
    own_out[...] = norm_rows(own[...].astype(F32), gain[...]).astype(BF16)
    other_out[...] = norm_rows(other[...].astype(F32), gain[...]).astype(BF16)


def pack_kernel(up, down, text, scale, out):
    out[0:64] = up[...]
    out[64:128] = down[...]
    out[128:224] = text[:, 0:512]
    out[224:272, 0:256] = text[0:48, 512:768]
    out[224:272, 256:512] = text[48:96, 512:768]
    out[272:288] = scale[...]


def unpack_kernel(m0, m1, m2, m3, ups, downs, texts, scales):
    for r, m in enumerate((m0, m1, m2, m3)):
        ups[r * 64 : (r + 1) * 64] = m[0:64]
        downs[r * 64 : (r + 1) * 64] = m[64:128]
        texts[r * 96 : (r + 1) * 96, 0:512] = m[128:224]
        texts[r * 96 : r * 96 + 48, 512:768] = m[224:272, 0:256]
        texts[r * 96 + 48 : (r + 1) * 96, 512:768] = m[224:272, 256:512]
        scales[r * 8 : (r + 1) * 8] = jnp.broadcast_to(
            jnp.sum(m[272:288, 0:128].astype(F32), axis=0, keepdims=True), (8, 128)
        )


def join_kernel(a, b, c, d, out):
    for r, part in enumerate((a, b, c, d)):
        out[r * 256 : (r + 1) * 256] = part[...]


def interleave_kernel(a, b, c, d, out):
    for r, part in enumerate((a, b, c, d)):
        for k in range(4):
            out[(k * 4 + r) * 64 : (k * 4 + r + 1) * 64] = part[k * 64 : (k + 1) * 64]


def attend_kernel(own, other, piece, scales, out):
    scale = scales[0:1]
    ones = block_ones(256, 64)
    lane = lax.broadcasted_iota(jnp.int32, (64, 128), 1)
    first = lane < 64
    nil = jnp.zeros((64, 128), F32)
    for side, rows in enumerate((own, other)):
        joint = jnp.dot(rows[...], piece[:, 0:384], preferred_element_type=F32)
        pair = joint[:, 0:256]
        high, low = split(pair * pair)
        squares = jnp.dot(high, ones, preferred_element_type=F32) + jnp.dot(low, ones, preferred_element_type=F32)
        unit = pair * lax.rsqrt(squares + 1e-06)
        for i in range(6):
            at = slice(i * 64, (i + 1) * 64)
            query = unit[at, 0:128].astype(BF16)
            key = unit[at, 128:256]
            value = joint[at, 256:384]
            keys = jnp.concatenate([jnp.where(first, key, nil), jnp.where(first, nil, key)], axis=0).astype(BF16)
            values = jnp.concatenate([jnp.where(first, value, nil), jnp.where(first, nil, value)], axis=0).astype(BF16)
            scores = lax.dot_general(query, keys, NT, preferred_element_type=F32)
            weights = jnp.exp(scores * scale).astype(BF16)
            mixed = jnp.dot(weights, values, preferred_element_type=F32)
            total = jnp.dot(weights, ones[0:128, 0:128], preferred_element_type=F32)
            out[side * 384 + i * 64 : side * 384 + (i + 1) * 64, :] = (mixed / total).astype(BF16)


def output_kernel(h0, h1, h2, h3, p0, p1, p2, p3, own, other):
    heads = jnp.concatenate([h0[...], h1[...], h2[...], h3[...]], axis=1)
    weight = jnp.concatenate([p0[...], p1[...], p2[...], p3[...]], axis=1)
    own[...] = lax.dot_general(heads[0:384], weight, NT, preferred_element_type=F32)
    other[...] = lax.dot_general(heads[384:768], weight, NT, preferred_element_type=F32).astype(BF16)


def residual_kernel(patches, own, other, gain, normed, pooled):
    residual = patches[...].astype(F32) + own[...] + other[...].astype(F32)
    normed[...] = norm_rows(residual, gain[...]).astype(BF16)
    pooled[0:6] = jnp.sum(residual.reshape(6, 64, 1024), axis=1) * (1.0 / 64)
    pooled[6:8] = jnp.zeros((2, 1024), F32)


def up_kernel(place, own, other, p0, p1, p2, p3, mean, weight):
    for r, piece in enumerate((p0, p1, p2, p3)):
        for j in range(4):
            at = pl.multiple_of(place[r * 4 + j] * 64, 64)
            weight[pl.ds(at, 64), :] = piece[j * 64 : (j + 1) * 64, :]
    for side, rows in enumerate((own, other)):
        upper = jnp.dot(rows[...], weight[...], preferred_element_type=F32)
        hidden = (0.5 * upper * (1.0 + lax.erf(upper * 0.7071067811865476))).astype(BF16).astype(F32)
        mean[side * 8 : side * 8 + 6, :] = jnp.sum(hidden.reshape(6, 64, 512), axis=1) * (1.0 / 64)
        mean[side * 8 + 6 : side * 8 + 8, :] = jnp.zeros((2, 512), F32)


def down_kernel(place, mean, p0, p1, p2, p3, own, other, weight):
    for r, piece in enumerate((p0, p1, p2, p3)):
        for j in range(4):
            at = pl.multiple_of(place[r * 4 + j] * 64, 64)
            for k in range(4):
                weight[pl.ds(at, 64), k * 512 : (k + 1) * 512] = piece[(j * 4 + k) * 64 : (j * 4 + k + 1) * 64, :]
    high, low = split(mean[...])
    both = jnp.concatenate([high, low], axis=0)
    product = lax.dot_general(both, weight[...], NT, preferred_element_type=F32)
    product = product[0:16] + product[16:32]
    own[...] = product[0:8]
    other[...] = product[8:16]


def final_kernel(pooled, own, other, gain, project, units):
    total = pooled[...] + own[...] + other[...]
    normed = norm_rows(total, gain[...]).astype(BF16)
    embedded = jnp.dot(normed, project[...], preferred_element_type=F32)
    units[...] = (
        embedded * lax.rsqrt(jnp.sum(embedded * embedded, axis=-1, keepdims=True) + 1e-06)
    ).astype(BF16)


def logits_kernel(units, texts, wanted, ids, out):
    logits = lax.dot_general(units[...], texts[...], NT, preferred_element_type=F32)
    highest = jnp.max(logits, axis=1, keepdims=True)
    total = jnp.sum(jnp.exp(logits - highest), axis=1, keepdims=True)
    matched = jnp.sum(jnp.where(wanted[...] == ids[...], logits, 0.0), axis=1, keepdims=True)
    lane = lax.broadcasted_iota(jnp.int32, (128, 128), 1)
    out[...] = jnp.where(lane == 0, highest, jnp.where(lane == 1, total, matched))


def loss_kernel(parts, loss):
    highest = parts[0]
    for i in range(1, 16):
        highest = jnp.maximum(highest, parts[i])
    highest = highest[:, 0:1]
    total = jnp.zeros((8, 1), F32)
    matched = jnp.zeros((8, 1), F32)
    for i in range(16):
        part = parts[i]
        total = total + part[:, 1:2] * jnp.exp(part[:, 0:1] - highest)
        matched = matched + part[:, 2:3]
    loss[...] = jnp.broadcast_to(highest + jnp.log(total) - matched, (8, 128))


def shards(
    patches,
    gain_first,
    joint_weight,
    head_scale,
    output_weight,
    gain_second,
    up_weight,
    down_weight,
    gain_final,
    project_weight,
    text_bank,
    captions,
    reference_loss,
):
    dp, mp = lax.axis_index("dp"), lax.axis_index("mp")
    ix, iy, iz, core = dp // 4, dp % 4, mp // 2, mp % 2
    sign = 1 - 2 * core
    offsets = jnp.stack([0 * sign, -sign, sign, 0 * sign + 2])
    rx, ry, rz = (ix + offsets + 4) % 4, (iy + offsets + 4) % 4, (iz + offsets + 4) % 4
    by_y_x = (rx[None, :] * 4 + ry[:, None]).reshape(16).astype(jnp.int32)
    by_x_y = (rx[:, None] * 4 + ry[None, :]).reshape(16).astype(jnp.int32)

    rows = patches.reshape(384, 1024)
    rows_other = swapped(rows)
    sds = jax.ShapeDtypeStruct

    lanes = jnp.repeat(head_scale, 64)
    high = lax.reduce_precision(lanes, 8, 7)
    middle = lax.reduce_precision(lanes - high, 8, 7)
    low = lanes - high - middle
    scale_rows = jnp.pad(jnp.stack([high, middle, low]), ((0, 13), (0, 384))).astype(BF16)
    message = call(pack_kernel, [sds((288, 512), BF16)], [up_weight, down_weight.T, text_bank, scale_rows])[0]
    messages = ring(message, 2)
    shard_a = jnp.concatenate([joint_weight.reshape(64, 384), output_weight.T], axis=1)
    plane_a = lax.all_to_all(jnp.broadcast_to(shard_a[None], (16, 64, 512)), "dp", 0, 0, tiled=True)
    pieces_a = ring(plane_a.reshape(1024, 512), 2)
    first_b, first_c, texts_own, scales = call(
        unpack_kernel,
        [sds((256, 512), BF16), sds((256, 512), BF16), sds((384, 768), BF16), sds((32, 128), F32)],
        messages,
    )
    second_b = call(interleave_kernel, [sds((1024, 512), BF16)], ring(first_b, 1))[0]
    second_c = call(join_kernel, [sds((1024, 512), BF16)], ring(first_c, 0))[0]
    pieces_b = ring(second_b, 0)
    pieces_c = ring(second_c, 1)
    texts = jnp.concatenate([texts_own, swapped(texts_own)], axis=0)

    gain_row = gain_first.reshape(1, 1024)
    normed_own, normed_other = call(norm_kernel, [sds((384, 1024), BF16)] * 2, [rows, rows_other, gain_row])
    heads = []
    for r, piece in enumerate(pieces_a):
        heads += call(
            attend_kernel,
            [sds((768, 128), BF16)],
            [normed_own, normed_other, piece, scales],
            ins=[None, None, None, pl.BlockSpec((8, 128), lambda *_, r=r: (r, 0))],
        )
    last = pl.BlockSpec((1024, 128), lambda *_: (0, 3))
    part_own, part_other = call(
        output_kernel, [sds((384, 1024), F32), sds((384, 1024), BF16)], [*heads, *pieces_a], ins=[None] * 4 + [last] * 4
    )
    normed_two, pooled = call(
        residual_kernel,
        [sds((384, 1024), BF16), sds((8, 1024), F32)],
        [rows, part_own, swapped(part_other), gain_second.reshape(1, 1024)],
    )
    quarter = pl.BlockSpec((256, 512), lambda i, *_: (i, 0))
    mean = call(
        up_kernel,
        [sds((16, 2048), F32)],
        [by_x_y, normed_two, swapped(normed_two), *pieces_b],
        grid=(4,),
        ins=[None] * 2 + [quarter] * 4,
        out_specs=[pl.BlockSpec((16, 512), lambda i, *_: (0, i))],
        scratch=[pltpu.VMEM((1024, 512), BF16)],
        prefetch=1,
    )[0]
    feed_own, feed_other = call(
        down_kernel,
        [sds((8, 1024), F32)] * 2,
        [by_y_x, mean, *pieces_c],
        scratch=[pltpu.VMEM((1024, 2048), BF16)],
        limit=24,
        prefetch=1,
    )
    units = call(
        final_kernel,
        [sds((8, 768), BF16)],
        [pooled, feed_own, swapped(feed_other), gain_final.reshape(1, 1024), project_weight],
    )[0]

    rz_other = (iz - offsets + 4) % 4
    holders = jnp.concatenate([rz * 2 + core, rz_other * 2 + (1 - core)])
    ids = ((dp * 8 + holders)[:, None] * 96 + jnp.arange(96)[None, :]).reshape(1, 768).astype(jnp.int32)
    wanted = lax.dynamic_slice_in_dim(captions.reshape(16, 8, 6), mp, 1, axis=1)[:, 0]
    wanted = jnp.pad(wanted, ((0, 0), (0, 2)), constant_values=-1).reshape(128, 1)

    everyone = lax.all_to_all(jnp.broadcast_to(units[None], (16, 8, 768)), "dp", 0, 0, tiled=True)
    parts = call(logits_kernel, [sds((128, 128), F32)], [everyone.reshape(128, 768), texts, wanted, ids])[0]
    parts = lax.all_to_all(parts.reshape(16, 8, 128), "dp", 0, 0, tiled=True)
    loss = call(loss_kernel, [sds((8, 128), F32)], [parts])[0]
    return loss[0:6, 0] - reference_loss


def solution(mesh):
    placed = (
        P(("dp", "mp"), None, None),
        P(),
        P("dp", None, "mp"),
        P("mp"),
        P("mp", "dp"),
        P(),
        P("dp", "mp"),
        P("mp", "dp"),
        P(),
        P(),
        P(("dp", "mp"), None),
        P(),
        P(("dp", "mp")),
    )

    return jax.shard_map(shards, mesh=mesh, in_specs=placed, out_specs=P(("dp", "mp")), check_vma=False)
```

```python
import jax
import jax.numpy as jnp
from jax import lax
from jax.experimental import pallas as pl
from jax.experimental.pallas import tpu as pltpu
from jax.sharding import PartitionSpec as P


AXES = ("dp", "mp")
DEVICES = [(x, y, z, c) for x in range(4) for y in range(4) for z in range(4) for c in range(2)]
F32 = jnp.float32
BF16 = jnp.bfloat16
NT = (((1,), (1,)), ((), ()))


def device_id(x, y, z, c):
    return x * 32 + y * 8 + z * 2 + c


def shift_pairs(axis, step):
    pairs = []
    for place in DEVICES:
        goal = list(place)
        goal[axis] = (goal[axis] + (step if place[3] == 0 else -step)) % 4
        pairs.append((device_id(*place), device_id(*goal)))
    return pairs


SWAP = [(i, i ^ 1) for i in range(128)]


def swapped(array):
    return lax.ppermute(array, AXES, SWAP)


def ring(array, axis):
    ahead = lax.ppermute(array, AXES, shift_pairs(axis, 1))
    behind = lax.ppermute(array, AXES, shift_pairs(axis, -1))
    far = lax.ppermute(ahead, AXES, shift_pairs(axis, 1))
    return [array, ahead, behind, far]


def call(body, outs, args, grid=(1,), ins=None, out_specs=None, scratch=(), prefetch=0, limit=16):
    whole = lambda s: pl.BlockSpec(s, lambda *_: (0,) * len(s))
    ins = ins or [None] * (len(args) - prefetch)
    ins = [b or whole(a.shape) for b, a in zip(ins, args[prefetch:])]
    out_specs = out_specs or [whole(o.shape) for o in outs]
    return pl.pallas_call(
        body,
        out_shape=outs,
        grid_spec=pltpu.PrefetchScalarGridSpec(
            num_scalar_prefetch=prefetch, grid=grid, in_specs=ins, out_specs=out_specs, scratch_shapes=list(scratch)
        ),
        compiler_params=pltpu.CompilerParams(vmem_limit_bytes=limit << 20),
    )(*args)


def norm_rows(values, gain):
    centre = values - jnp.mean(values, axis=-1, keepdims=True)
    spread = jnp.mean(centre * centre, axis=-1, keepdims=True)
    return centre * lax.rsqrt(spread + 1e-06) * gain


def split(values):
    high = values.astype(BF16)
    return high, (values - high.astype(F32)).astype(BF16)


def block_ones(size, block):
    row = lax.broadcasted_iota(jnp.int32, (size, size), 0) // block
    col = lax.broadcasted_iota(jnp.int32, (size, size), 1) // block
    return (row == col).astype(F32).astype(BF16)


def norm_kernel(own, other, gain, own_out, other_out):
    own_out[...] = norm_rows(own[...].astype(F32), gain[...]).astype(BF16)
    other_out[...] = norm_rows(other[...].astype(F32), gain[...]).astype(BF16)


def spread_kernel(joint, output, out):
    row = jnp.concatenate([joint[0], joint[1], joint[2], output[...]], axis=1)
    for d in range(16):
        out[d] = row


def pack_kernel(scale, up, down, text, out, sems):
    copies = [
        pltpu.make_async_copy(up, out.at[0:64], sems.at[0]),
        pltpu.make_async_copy(down, out.at[64:128], sems.at[1]),
        pltpu.make_async_copy(text.at[:, 0:512], out.at[128:224], sems.at[2]),
        pltpu.make_async_copy(text.at[0:48, 512:768], out.at[224:272, 0:256], sems.at[3]),
        pltpu.make_async_copy(text.at[48:96, 512:768], out.at[224:272, 256:512], sems.at[4]),
    ]
    for copy in copies:
        copy.start()
    lane = lax.broadcasted_iota(jnp.int32, (16, 512), 1)
    row = lax.broadcasted_iota(jnp.int32, (16, 512), 0)
    value = jnp.where(lane < 64, scale[0], scale[1])
    high = value.astype(BF16).astype(F32)
    middle = (value - high).astype(BF16).astype(F32)
    low = value - high - middle
    out[272:288] = jnp.where(
        row == 0, high, jnp.where(row == 1, middle, jnp.where(row == 2, low, 0.0))
    ).astype(BF16)
    for copy in copies:
        copy.wait()


def unpack_kernel(m0, m1, m2, m3, ups, downs, texts, scales):
    for r, m in enumerate((m0, m1, m2, m3)):
        ups[r * 64 : (r + 1) * 64] = m[0:64]
        downs[r * 64 : (r + 1) * 64] = m[64:128]
        texts[r * 96 : (r + 1) * 96, 0:512] = m[128:224]
        texts[r * 96 : r * 96 + 48, 512:768] = m[224:272, 0:256]
        texts[r * 96 + 48 : (r + 1) * 96, 512:768] = m[224:272, 256:512]
        scales[r * 8 : (r + 1) * 8] = jnp.broadcast_to(
            jnp.sum(m[272:288, 0:128].astype(F32), axis=0, keepdims=True), (8, 128)
        )


def interleave_kernel(a, b, c, d, out):
    for r, part in enumerate((a, b, c, d)):
        for k in range(4):
            out[(k * 4 + r) * 64 : (k * 4 + r + 1) * 64] = part[k * 64 : (k + 1) * 64]


def attend_kernel(own, other, piece, scales, out):
    scale = scales[0:1]
    ones = block_ones(256, 64)
    lane = lax.broadcasted_iota(jnp.int32, (64, 128), 1)
    first = lane < 64
    nil = jnp.zeros((64, 128), F32)
    for side, rows in enumerate((own, other)):
        joint = jnp.dot(rows[...], piece[:, 0:384], preferred_element_type=F32)
        pair = joint[:, 0:256]
        high, low = split(pair * pair)
        squares = jnp.dot(high, ones, preferred_element_type=F32) + jnp.dot(low, ones, preferred_element_type=F32)
        unit = pair * lax.rsqrt(squares + 1e-06)
        for i in range(6):
            at = slice(i * 64, (i + 1) * 64)
            query = unit[at, 0:128].astype(BF16)
            key = unit[at, 128:256]
            value = joint[at, 256:384]
            keys = jnp.concatenate([jnp.where(first, key, nil), jnp.where(first, nil, key)], axis=0).astype(BF16)
            values = jnp.concatenate([jnp.where(first, value, nil), jnp.where(first, nil, value)], axis=0).astype(BF16)
            scores = lax.dot_general(query, keys, NT, preferred_element_type=F32)
            weights = jnp.exp(scores * scale).astype(BF16)
            mixed = jnp.dot(weights, values, preferred_element_type=F32)
            total = jnp.dot(weights, ones[0:128, 0:128], preferred_element_type=F32)
            out[side * 384 + i * 64 : side * 384 + (i + 1) * 64, :] = (mixed / total).astype(BF16)


def output_kernel(h0, h1, h2, h3, p0, p1, p2, p3, own, other):
    heads = jnp.concatenate([h0[...], h1[...], h2[...], h3[...]], axis=1)
    weight = jnp.concatenate([p0[...], p1[...], p2[...], p3[...]], axis=1)
    own[...] = lax.dot_general(heads[0:384], weight, NT, preferred_element_type=F32)
    other[...] = lax.dot_general(heads[384:768], weight, NT, preferred_element_type=F32).astype(BF16)


def residual_kernel(patches, own, other, gain, normed, pooled):
    residual = patches[...].astype(F32) + own[...] + other[...].astype(F32)
    normed[...] = norm_rows(residual, gain[...]).astype(BF16)
    pooled[0:6] = jnp.sum(residual.reshape(6, 64, 1024), axis=1) * (1.0 / 64)
    pooled[6:8] = jnp.zeros((2, 1024), F32)


def up_kernel(place, own, other, p0, p1, p2, p3, mean, weight):
    for r, piece in enumerate((p0, p1, p2, p3)):
        for j in range(4):
            at = pl.multiple_of(place[r * 4 + j] * 64, 64)
            weight[pl.ds(at, 64), :] = piece[j * 64 : (j + 1) * 64, :]
    for side, rows in enumerate((own, other)):
        upper = jnp.dot(rows[...], weight[...], preferred_element_type=F32)
        hidden = (0.5 * upper * (1.0 + lax.erf(upper * 0.7071067811865476))).astype(BF16).astype(F32)
        mean[side * 8 : side * 8 + 6, :] = jnp.sum(hidden.reshape(6, 64, 512), axis=1) * (1.0 / 64)
        mean[side * 8 + 6 : side * 8 + 8, :] = jnp.zeros((2, 512), F32)


def down_kernel(place, mean, p0, p1, p2, p3, own, other):
    high, low = split(mean[...])
    both = jnp.concatenate([high, low], axis=0)
    for r, piece in enumerate((p0, p1, p2, p3)):
        product = jnp.zeros((32, 256), F32)
        for k in range(4):
            product = product + lax.dot_general(
                both[:, k * 512 : (k + 1) * 512],
                piece[k * 256 : (k + 1) * 256, :],
                NT,
                preferred_element_type=F32,
            )
        product = product[0:16] + product[16:32]
        for j in range(4):
            own[place[r * 4 + j]] = product[0:8, j * 64 : (j + 1) * 64]
            other[place[r * 4 + j]] = product[8:16, j * 64 : (j + 1) * 64]


def final_kernel(pooled, own, other, gain, project, units):
    feed = jnp.concatenate([own[d] + other[d] for d in range(16)], axis=1)
    normed = norm_rows(pooled[...] + feed, gain[...]).astype(BF16)
    embedded = jnp.dot(normed, project[...], preferred_element_type=F32)
    unit = (embedded * lax.rsqrt(jnp.sum(embedded * embedded, axis=-1, keepdims=True) + 1e-06)).astype(BF16)
    for d in range(16):
        units[d] = unit


def logits_kernel(units, texts, texts_other, wanted, ids, out):
    image = units[...]
    logits = jnp.concatenate(
        [lax.dot_general(image, t[...], NT, preferred_element_type=F32) for t in (texts, texts_other)], axis=1
    )
    highest = jnp.max(logits, axis=1, keepdims=True)
    total = jnp.sum(jnp.exp(logits - highest), axis=1, keepdims=True)
    matched = jnp.sum(jnp.where(wanted[...] == ids[...], logits, 0.0), axis=1, keepdims=True)
    lane = lax.broadcasted_iota(jnp.int32, (128, 128), 1)
    out[...] = jnp.where(lane == 0, highest, jnp.where(lane == 1, total, matched))


def loss_kernel(parts, loss):
    highest = parts[0]
    for i in range(1, 16):
        highest = jnp.maximum(highest, parts[i])
    highest = highest[:, 0:1]
    total = jnp.zeros((8, 1), F32)
    matched = jnp.zeros((8, 1), F32)
    for i in range(16):
        part = parts[i]
        total = total + part[:, 1:2] * jnp.exp(part[:, 0:1] - highest)
        matched = matched + part[:, 2:3]
    loss[...] = jnp.broadcast_to(highest + jnp.log(total) - matched, (8, 128))


def shards(
    patches,
    gain_first,
    joint_weight,
    head_scale,
    output_weight,
    gain_second,
    up_weight,
    down_weight,
    gain_final,
    project_weight,
    text_bank,
    captions,
    reference_loss,
):
    dp, mp = lax.axis_index("dp"), lax.axis_index("mp")
    ix, iy, iz, core = dp // 4, dp % 4, mp // 2, mp % 2
    sign = 1 - 2 * core
    offsets = jnp.stack([0 * sign, -sign, sign, 0 * sign + 2])
    rx, ry, rz = (ix + offsets + 4) % 4, (iy + offsets + 4) % 4, (iz + offsets + 4) % 4
    by_y_x = (rx[None, :] * 4 + ry[:, None]).reshape(16).astype(jnp.int32)
    by_x_y = (rx[:, None] * 4 + ry[None, :]).reshape(16).astype(jnp.int32)

    rows = patches.reshape(384, 1024)
    rows_other = swapped(rows)
    sds = jax.ShapeDtypeStruct

    spread = call(spread_kernel, [sds((16, 64, 512), BF16)], [jnp.moveaxis(joint_weight, 1, 0), output_weight.T])[0]
    anywhere = pl.BlockSpec(memory_space=pl.ANY)
    message = call(
        pack_kernel,
        [sds((288, 512), BF16)],
        [head_scale, up_weight, down_weight.T, text_bank],
        ins=[anywhere] * 3,
        scratch=[pltpu.SemaphoreType.DMA((5,))],
        prefetch=1,
    )[0]
    messages = ring(message, 2)
    plane_a = lax.all_to_all(spread, "dp", 0, 0, tiled=True)
    pieces_a = ring(plane_a.reshape(1024, 512), 2)
    first_b, first_c, texts_own, scales = call(
        unpack_kernel,
        [sds((256, 512), BF16), sds((256, 512), BF16), sds((384, 768), BF16), sds((32, 128), F32)],
        messages,
    )
    second_b = call(interleave_kernel, [sds((1024, 512), BF16)], ring(first_b, 1))[0]
    second_c = call(interleave_kernel, [sds((1024, 512), BF16)], ring(first_c, 0))[0]
    pieces_b = ring(second_b, 0)
    pieces_c = ring(second_c, 1)
    texts_other = swapped(texts_own)

    gain_row = gain_first.reshape(1, 1024)
    normed_own, normed_other = call(norm_kernel, [sds((384, 1024), BF16)] * 2, [rows, rows_other, gain_row])
    heads = []
    for r, piece in enumerate(pieces_a):
        heads += call(
            attend_kernel,
            [sds((768, 128), BF16)],
            [normed_own, normed_other, piece, scales],
            ins=[None, None, None, pl.BlockSpec((8, 128), lambda *_, r=r: (r, 0))],
        )
    last = pl.BlockSpec((1024, 128), lambda *_: (0, 3))
    part_own, part_other = call(
        output_kernel, [sds((384, 1024), F32), sds((384, 1024), BF16)], [*heads, *pieces_a], ins=[None] * 4 + [last] * 4
    )
    normed_two, pooled = call(
        residual_kernel,
        [sds((384, 1024), BF16), sds((8, 1024), F32)],
        [rows, part_own, swapped(part_other), gain_second.reshape(1, 1024)],
    )
    quarter = pl.BlockSpec((256, 512), lambda i, *_: (i, 0))
    mean = call(
        up_kernel,
        [sds((16, 2048), F32)],
        [by_x_y, normed_two, swapped(normed_two), *pieces_b],
        grid=(4,),
        ins=[None] * 2 + [quarter] * 4,
        out_specs=[pl.BlockSpec((16, 512), lambda i, *_: (0, i))],
        scratch=[pltpu.VMEM((1024, 512), BF16)],
        prefetch=1,
    )[0]
    feed_own, feed_other = call(
        down_kernel, [sds((16, 8, 64), F32)] * 2, [by_y_x, mean, *pieces_c], limit=24, prefetch=1
    )
    units = call(
        final_kernel,
        [sds((16, 8, 768), BF16)],
        [pooled, feed_own, swapped(feed_other), gain_final.reshape(1, 1024), project_weight],
    )[0]

    rz_other = (iz - offsets + 4) % 4
    holders = jnp.concatenate([rz * 2 + core, rz_other * 2 + (1 - core)])
    ids = ((dp * 8 + holders)[:, None] * 96 + jnp.arange(96)[None, :]).reshape(1, 768).astype(jnp.int32)
    wanted = lax.dynamic_slice_in_dim(captions.reshape(16, 8, 6), mp, 1, axis=1)[:, 0]
    wanted = jnp.pad(wanted, ((0, 0), (0, 2)), constant_values=-1).reshape(128, 1)

    everyone = lax.all_to_all(units, "dp", 0, 0, tiled=True)
    parts = call(
        logits_kernel, [sds((128, 128), F32)], [everyone.reshape(128, 768), texts_own, texts_other, wanted, ids]
    )[0]
    parts = lax.all_to_all(parts.reshape(16, 8, 128), "dp", 0, 0, tiled=True)
    loss = call(loss_kernel, [sds((8, 128), F32)], [parts])[0]
    return loss[0:6, 0] - reference_loss


def solution(mesh):
    placed = (
        P(("dp", "mp"), None, None),
        P(),
        P("dp", None, "mp"),
        P("mp"),
        P("mp", "dp"),
        P(),
        P("dp", "mp"),
        P("mp", "dp"),
        P(),
        P(),
        P(("dp", "mp"), None),
        P(),
        P(("dp", "mp")),
    )

    return jax.shard_map(shards, mesh=mesh, in_specs=placed, out_specs=P(("dp", "mp")), check_vma=False)
```

```python
import jax
import jax.numpy as jnp
from jax import lax
from jax.experimental import pallas as pl
from jax.experimental.pallas import tpu as pltpu
from jax.sharding import Mesh, PartitionSpec as P


AXES = ("x", "y", "z", "core")
DEVICES = [(x, y, z, c) for x in range(4) for y in range(4) for z in range(4) for c in range(2)]
F32 = jnp.float32
BF16 = jnp.bfloat16
NT = (((1,), (1,)), ((), ()))


def device_id(x, y, z, c):
    return x * 32 + y * 8 + z * 2 + c


def shift_pairs(axis, step):
    pairs = []
    for place in DEVICES:
        goal = list(place)
        goal[axis] = (goal[axis] + (step if place[3] == 0 else -step)) % 4
        pairs.append((device_id(*place), device_id(*goal)))
    return pairs


SWAP = [(i, i ^ 1) for i in range(128)]


def swapped(array):
    return lax.ppermute(array, AXES, SWAP)


def ring(array, axis, direct=False):
    ahead = lax.ppermute(array, AXES, shift_pairs(axis, 1))
    behind = lax.ppermute(array, AXES, shift_pairs(axis, -1))
    if direct:
        far = lax.ppermute(array, AXES, shift_pairs(axis, 2))
    else:
        far = lax.ppermute(ahead, AXES, shift_pairs(axis, 1))
    return [array, ahead, behind, far]


def call(body, outs, args, grid=(1,), ins=None, out_specs=None, scratch=(), prefetch=0, limit=16):
    whole = lambda s: pl.BlockSpec(s, lambda *_: (0,) * len(s))
    ins = ins or [None] * (len(args) - prefetch)
    ins = [b or whole(a.shape) for b, a in zip(ins, args[prefetch:])]
    out_specs = out_specs or [whole(o.shape) for o in outs]
    return pl.pallas_call(
        body,
        out_shape=outs,
        grid_spec=pltpu.PrefetchScalarGridSpec(
            num_scalar_prefetch=prefetch, grid=grid, in_specs=ins, out_specs=out_specs, scratch_shapes=list(scratch)
        ),
        compiler_params=pltpu.CompilerParams(vmem_limit_bytes=limit << 20),
    )(*args)


def norm_rows(values, gain):
    centre = values - jnp.mean(values, axis=-1, keepdims=True)
    spread = jnp.mean(centre * centre, axis=-1, keepdims=True)
    return centre * lax.rsqrt(spread + 1e-06) * gain


def nearby():
    sign = 1 - 2 * lax.axis_index("core")
    offsets = (0, -sign, sign, 2)
    return [[(lax.axis_index(axis) + offset) & 3 for offset in offsets] for axis in AXES[:3]]


def split(values):
    high = values.astype(BF16)
    return high, (values - high.astype(F32)).astype(BF16)


def block_ones(size, block):
    row = lax.broadcasted_iota(jnp.int32, (size, size), 0) // block
    col = lax.broadcasted_iota(jnp.int32, (size, size), 1) // block
    return (row == col).astype(F32).astype(BF16)


def norm_kernel(own, other, gain, own_out, other_out):
    own_out[...] = norm_rows(own[...].astype(F32), gain[...]).astype(BF16)
    other_out[...] = norm_rows(other[...].astype(F32), gain[...]).astype(BF16)


def unpack_kernel(m0, m1, m2, m3, ups, downs):
    for r, m in enumerate((m0, m1, m2, m3)):
        ups[r * 64 : (r + 1) * 64] = m[0:64]
        downs[r * 64 : (r + 1) * 64] = m[64:128]


def join_kernel(a, b, c, d, out):
    size = a.shape[0]
    for r, part in enumerate((a, b, c, d)):
        out[r * size : (r + 1) * size] = part[...]


def interleave_kernel(a, b, c, d, out):
    for r, part in enumerate((a, b, c, d)):
        for k in range(4):
            out[(k * 4 + r) * 64 : (k * 4 + r + 1) * 64] = part[k * 64 : (k + 1) * 64]


def settle_kernel(scale, a, b, c, d, out):
    xs, ys, _ = nearby()
    for r, part in enumerate((a, b, c, d)):
        for k in range(4):
            at = pl.multiple_of((xs[k] * 4 + ys[r]) * 64, 64)
            out[pl.ds(at, 64), :] = part[k * 64 : (k + 1) * 64]
    lane = lax.broadcasted_iota(jnp.int32, (16, 512), 1)
    row = lax.broadcasted_iota(jnp.int32, (16, 512), 0)
    value = jnp.where(lane < 64, scale[0], scale[1])
    high = value.astype(BF16).astype(F32)
    middle = (value - high).astype(BF16).astype(F32)
    low = value - high - middle
    out[1024:1040] = jnp.where(
        row == 0, high, jnp.where(row == 1, middle, jnp.where(row == 2, low, 0.0))
    ).astype(BF16)


def attend_kernel(own, other, piece, out):
    scale = jnp.sum(piece[1024:1040, 0:128].astype(F32), axis=0, keepdims=True)
    ones = block_ones(256, 64)
    lane = lax.broadcasted_iota(jnp.int32, (64, 128), 1)
    first = lane < 64
    nil = jnp.zeros((64, 128), F32)
    for side, rows in enumerate((own, other)):
        joint = jnp.dot(rows[...], piece[0:1024, 0:384], preferred_element_type=F32)
        pair = joint[:, 0:256]
        high, low = split(pair * pair)
        squares = jnp.dot(high, ones, preferred_element_type=F32) + jnp.dot(low, ones, preferred_element_type=F32)
        unit = pair * lax.rsqrt(squares + 1e-06)
        for i in range(6):
            at = slice(i * 64, (i + 1) * 64)
            query = unit[at, 0:128].astype(BF16)
            key = unit[at, 128:256]
            value = joint[at, 256:384]
            keys = jnp.concatenate([jnp.where(first, key, nil), jnp.where(first, nil, key)], axis=0).astype(BF16)
            values = jnp.concatenate([jnp.where(first, value, nil), jnp.where(first, nil, value)], axis=0).astype(BF16)
            scores = lax.dot_general(query, keys, NT, preferred_element_type=F32)
            weights = jnp.exp(scores * scale).astype(BF16)
            mixed = jnp.dot(weights, values, preferred_element_type=F32)
            total = jnp.dot(weights, ones[0:128, 0:128], preferred_element_type=F32)
            out[side * 384 + i * 64 : side * 384 + (i + 1) * 64, :] = (mixed / total).astype(BF16)


def output_kernel(h0, h1, h2, h3, p0, p1, p2, p3, own, other):
    heads = jnp.concatenate([h0[...], h1[...], h2[...], h3[...]], axis=1)
    weight = jnp.concatenate([p0[...], p1[...], p2[...], p3[...]], axis=1)
    own[...] = lax.dot_general(heads[0:384], weight, NT, preferred_element_type=F32)
    other[...] = lax.dot_general(heads[384:768], weight, NT, preferred_element_type=F32).astype(BF16)


def residual_kernel(patches, own, other, gain, normed, pooled):
    residual = patches[...].astype(F32) + own[...] + other[...].astype(F32)
    normed[...] = norm_rows(residual, gain[...]).astype(BF16)
    pooled[0:6] = jnp.sum(residual.reshape(6, 64, 1024), axis=1) * (1.0 / 64)
    pooled[6:8] = jnp.zeros((2, 1024), F32)


def up_kernel(own, other, p0, p1, p2, p3, mean, weight):
    xs, ys, _ = nearby()
    for r, piece in enumerate((p0, p1, p2, p3)):
        for j in range(4):
            at = pl.multiple_of((xs[j] * 4 + ys[r]) * 64, 64)
            weight[pl.ds(at, 64), :] = piece[j * 64 : (j + 1) * 64, :]
    for side, rows in enumerate((own, other)):
        upper = jnp.dot(rows[...], weight[...], preferred_element_type=F32)
        hidden = (0.5 * upper * (1.0 + lax.erf(upper * 0.7071067811865476))).astype(BF16).astype(F32)
        mean[side * 8 : side * 8 + 6, :] = jnp.sum(hidden.reshape(6, 64, 512), axis=1) * (1.0 / 64)
        mean[side * 8 + 6 : side * 8 + 8, :] = jnp.zeros((2, 512), F32)


def down_kernel(mean, p0, p1, p2, p3, own, other):
    xs, ys, _ = nearby()
    high, low = split(mean[...])
    both = jnp.concatenate([high, low], axis=0)
    for r, piece in enumerate((p0, p1, p2, p3)):
        product = jnp.zeros((32, 256), F32)
        for k in range(4):
            product = product + lax.dot_general(
                both[:, k * 512 : (k + 1) * 512],
                piece[k * 256 : (k + 1) * 256, :],
                NT,
                preferred_element_type=F32,
            )
        product = product[0:16] + product[16:32]
        for j in range(4):
            own[xs[r] * 4 + ys[j]] = product[0:8, j * 64 : (j + 1) * 64]
            other[xs[r] * 4 + ys[j]] = product[8:16, j * 64 : (j + 1) * 64]


def final_kernel(pooled, own, other, gain, project, units):
    feed = jnp.concatenate([own[d] + other[d] for d in range(16)], axis=1)
    normed = norm_rows(pooled[...] + feed, gain[...]).astype(BF16)
    embedded = jnp.dot(normed, project[...], preferred_element_type=F32)
    unit = (embedded * lax.rsqrt(jnp.sum(embedded * embedded, axis=-1, keepdims=True) + 1e-06)).astype(BF16)
    for d in range(16):
        units[d] = unit


def logits_kernel(captions, units, texts, texts_other, out):
    image = units[...]
    core = lax.axis_index("core")
    xs = nearby()[0]
    place = lax.axis_index("y") * 8 + lax.axis_index("z") * 2
    column = lax.broadcasted_iota(jnp.int32, (1, 384), 1)
    logits, ids = [], []
    for rows, order, side in ((texts, (0, 1, 2, 3), core), (texts_other, (0, 2, 1, 3), 1 - core)):
        logits.append(lax.dot_general(image, rows[...], NT, preferred_element_type=F32))
        spot = column
        for block, r in enumerate(order):
            holder = (xs[r] * 32 + place + side) * 96 - block * 96
            inside = (column >= block * 96) & (column < block * 96 + 96)
            spot = jnp.where(inside, column + holder, spot)
        ids.append(spot)
    logits, ids = jnp.concatenate(logits, axis=1), jnp.concatenate(ids, axis=1)
    row = lax.broadcasted_iota(jnp.int32, (8, 1), 0)
    wanted = []
    for d in range(16):
        part = jnp.full((8, 1), -1, jnp.int32)
        for k in range(6):
            part = jnp.where(row == k, captions[(lax.axis_index("x") * 32 + d * 2 + core) * 6 + k], part)
        wanted.append(part)
    wanted = jnp.concatenate(wanted, axis=0)
    highest = jnp.max(logits, axis=1, keepdims=True)
    total = jnp.sum(jnp.exp(logits - highest), axis=1, keepdims=True)
    matched = jnp.sum(jnp.where(wanted == ids, logits, 0.0), axis=1, keepdims=True)
    lane = lax.broadcasted_iota(jnp.int32, (128, 128), 1)
    out[...] = jnp.where(lane == 0, highest, jnp.where(lane == 1, total, matched))


def loss_kernel(parts, baseline, loss):
    highest = parts[0]
    for i in range(1, 16):
        highest = jnp.maximum(highest, parts[i])
    highest = highest[:, 0:1]
    total = jnp.zeros((8, 1), F32)
    matched = jnp.zeros((8, 1), F32)
    for i in range(16):
        part = parts[i]
        total = total + part[:, 1:2] * jnp.exp(part[:, 0:1] - highest)
        matched = matched + part[:, 2:3]
    value = highest + jnp.log(total) - matched
    row = lax.broadcasted_iota(jnp.int32, (8, 128), 0)
    lane = lax.broadcasted_iota(jnp.int32, (8, 128), 1)
    across = jnp.sum(jnp.where(row == lane, value, 0.0), axis=0)
    loss[...] = across[0:6] - baseline[...]


def shards(
    patches,
    gain_first,
    joint_weight,
    head_scale,
    output_weight,
    gain_second,
    up_weight,
    down_weight,
    gain_final,
    project_weight,
    text_bank,
    captions,
    reference_loss,
):
    rows = patches.reshape(384, 1024)
    rows_other = swapped(rows)
    sds = jax.ShapeDtypeStruct

    front = jnp.concatenate([joint_weight[:, part] for part in range(3)] + [output_weight.T], axis=1)
    message = jnp.concatenate([up_weight, down_weight.T], axis=0)
    small = dict(limit=6)
    first_a = call(join_kernel, [sds((256, 512), BF16)], ring(front, 0, direct=True), **small)[0]
    second_a = call(settle_kernel, [sds((1040, 512), BF16)], [head_scale, *ring(first_a, 1)], prefetch=1, **small)[0]
    pieces_a = ring(second_a, 2)
    messages = ring(message, 2)
    first_b, first_c = call(unpack_kernel, [sds((256, 512), BF16), sds((256, 512), BF16)], messages, limit=4)
    texts_own = call(join_kernel, [sds((384, 768), BF16)], ring(text_bank, 0), **small)[0]
    second_b = call(interleave_kernel, [sds((1024, 512), BF16)], ring(first_b, 0), limit=6)[0]
    second_c = call(interleave_kernel, [sds((1024, 512), BF16)], ring(first_c, 1), limit=6)[0]
    pieces_b = ring(second_b, 1)
    pieces_c = ring(second_c, 0)
    texts_other = swapped(texts_own)

    gain_row = gain_first.reshape(1, 1024)
    normed_own, normed_other = call(norm_kernel, [sds((384, 1024), BF16)] * 2, [rows, rows_other, gain_row], limit=8)
    heads = []
    for piece in pieces_a:
        heads += call(attend_kernel, [sds((768, 128), BF16)], [normed_own, normed_other, piece], limit=10)
    last = pl.BlockSpec((1024, 128), lambda *_: (0, 3))
    part_own, part_other = call(
        output_kernel, [sds((384, 1024), F32), sds((384, 1024), BF16)], [*heads, *pieces_a], ins=[None] * 4 + [last] * 4
    )
    normed_two, pooled = call(
        residual_kernel,
        [sds((384, 1024), BF16), sds((8, 1024), F32)],
        [rows, part_own, swapped(part_other), gain_second.reshape(1, 1024)],
        limit=12,
    )
    quarter = pl.BlockSpec((256, 512), lambda i, *_: (i, 0))
    mean = call(
        up_kernel,
        [sds((16, 2048), F32)],
        [normed_two, swapped(normed_two), *pieces_b],
        grid=(4,),
        ins=[None] * 2 + [quarter] * 4,
        out_specs=[pl.BlockSpec((16, 512), lambda i, *_: (0, i))],
        scratch=[pltpu.VMEM((1024, 512), BF16)],
    )[0]
    feed_own, feed_other = call(down_kernel, [sds((16, 8, 64), F32)] * 2, [mean, *pieces_c], limit=24)
    units = call(
        final_kernel,
        [sds((16, 8, 768), BF16)],
        [pooled, feed_own, swapped(feed_other), gain_final.reshape(1, 1024), project_weight],
    )[0]

    everyone = lax.all_to_all(units, ("y", "z"), 0, 0, tiled=True)
    parts = call(
        logits_kernel,
        [sds((128, 128), F32)],
        [captions, everyone.reshape(128, 768), texts_own, texts_other],
        prefetch=1,
    )[0]
    parts = lax.all_to_all(parts.reshape(16, 8, 128), ("y", "z"), 0, 0, tiled=True)
    return call(loss_kernel, [sds((6,), F32)], [parts, reference_loss])[0]


def solution(mesh):
    grid = Mesh(mesh.devices.reshape(4, 4, 4, 2), AXES)
    dp, mp = ("x", "y"), ("z", "core")
    placed = (
        P(AXES, None, None),
        P(),
        P(dp, None, mp),
        P(mp),
        P(mp, dp),
        P(),
        P(dp, mp),
        P(mp, dp),
        P(),
        P(),
        P(AXES, None),
        P(),
        P(AXES),
    )

    return jax.shard_map(shards, mesh=grid, in_specs=placed, out_specs=P(AXES), check_vma=False)
```
